32 devices in a mesh: dp: 4 (over z), blk: 2 (over y), head: 4 (over x, core).
Axes of the slice: x: 2, y: 2, z: 4, core: 2. Of those that a mesh axis runs over, the one named last changes fastest.
Arguments:
- queries: bfloat16 [4, 1024, 1024], P('dp', ('blk', 'head')), may hold values from -40 to 40
- keys_values: bfloat16 [4, 1024, 512], P('dp', ('blk', 'head')), may hold values from -40 to 40
- out_weight: bfloat16 [1024, 2048], P('head'), may hold values from -0.125 to 0.125
- cotangent: bfloat16 [4, 1024, 2048], P('dp', ('blk', 'head')), may hold values from -6 to 6
- passage_lengths: int32 [4, 32], P('dp'), may hold values from 1 to 64, 992 in all within a row
- causal_flags: int32 [4, 32], P('dp'), may hold values from 0 to 1
Outputs:
- attn: bfloat16 [4, 1024, 1024], P('dp', 'blk', 'head')
- grad_queries: bfloat16 [4, 1024, 1024], P('dp', 'blk', 'head')
- grad_keys_values: bfloat16 [4, 1024, 512], P('dp', 'blk', 'head')
- grad_out_weight: bfloat16 [1024, 2048], P('head')
The draws below stay inside these ranges and needn't reach their ends.
Inputs may be any that keep to these rules, and one draw needn't show every extreme that they name: `passage_lengths`: each row sums to 992; its largest entry is 64.
All inputs are finite; a program needn't handle non-finite values.
Results may differ from the reference program's by a relative error of at most 0.019.
Values may be sent and summed in bfloat16 or wider, within the bound.
A program may use at most 128 MiB of HBM per device.

```python
import math
import jax
import jax.numpy as jnp
import numpy as np
from jax import lax

D = 2048
QUERY_HEADS = 16
KEY_VALUE_HEADS = 4
HEAD_SIZE = 64
LISTS = 32
GROUPS = 4
SEQUENCE_LENGTH = 1024
PREFIX = 32
MOST = 64
N_BLK = 2


def draw_group(key):
    heads_per_group = QUERY_HEADS // KEY_VALUE_HEADS
    queries = jnp.clip(jax.random.normal(jax.random.fold_in(key, 101), (SEQUENCE_LENGTH, KEY_VALUE_HEADS, heads_per_group, HEAD_SIZE), jnp.float32), -5.0, 5.0)
    index_pairs = jnp.clip(jax.random.normal(jax.random.fold_in(key, 102), (SEQUENCE_LENGTH, KEY_VALUE_HEADS, 2 * HEAD_SIZE), jnp.float32), -5.0, 5.0)
    queries = jnp.clip(queries, -40.0, 40.0).reshape(SEQUENCE_LENGTH, QUERY_HEADS * HEAD_SIZE)
    index_pairs = jnp.clip(index_pairs, -40.0, 40.0).reshape(SEQUENCE_LENGTH, KEY_VALUE_HEADS * 2 * HEAD_SIZE)
    return (queries, index_pairs)


def draw_queries(key, part):
    drawn = jax.vmap(lambda index: draw_group(jax.random.fold_in(key, index))[0])(jnp.arange(GROUPS))
    return drawn.astype(jnp.bfloat16)


def draw_keys_values(key, part):
    drawn = jax.vmap(lambda index: draw_group(jax.random.fold_in(key, index))[1])(jnp.arange(GROUPS))
    return drawn.astype(jnp.bfloat16)


def place_ends(entries, rng, least, high):
    shape = entries.shape
    place = [jax.random.randint(jax.random.fold_in(rng, axis), (), 0, shape[axis]) for axis in range(len(shape))]
    entries = entries.at[tuple(place)].set(least)
    longest = shape.index(max(shape))
    place[longest] = (place[longest] + 1) % shape[longest]
    return entries.at[tuple(place)].set(high)


def levels(key, extent, split, smallest, high):
    factor_of, own = 1.0, jax.random.fold_in(key, 6)
    for axis_at, parts in split:
        heights = jnp.exp(jax.random.uniform(jax.random.fold_in(own, axis_at), (parts,), jnp.float32, smallest / len(split), high / len(split)))
        factor_of = factor_of * jnp.repeat(heights, extent[axis_at] // parts).reshape([-1 if axis == axis_at else 1 for axis in range(len(extent))])
    return factor_of


def profile(number_of, total, most, skew):
    portions = [(1 << 20) // math.isqrt(grade ** skew) + 1 for grade in range(2, number_of + 1)]
    spare, given = total - most - (number_of - 1), [1] * (number_of - 1)
    while spare > 0:
        candidates = [i for i in range(number_of - 1) if given[i] < most]
        pool, left = sum([portions[i] for i in candidates]), spare
        for i in candidates:
            addition = min(most - given[i], max(1, left * portions[i] // pool), spare)
            given[i] = given[i] + addition
            spare = spare - addition
    return np.array([most] + given)


def ragged_sizes(rng, number_of, total, limit, lean):
    if number_of == 2:
        one = jax.random.randint(rng, (), max(1, total - limit), min(limit, total - 1) + 1)
        return jnp.stack([one, total - one])
    sizes = jnp.asarray(profile(number_of, total, limit, lean), jnp.int32)
    couples = (number_of - 1) // 2
    giver, taker = sizes[1:1 + 2 * couples:2], sizes[2:2 + 2 * couples:2]
    margin = jnp.minimum(giver - 1, limit - taker)
    shifted = jax.random.randint(jax.random.fold_in(rng, 1), (couples,), 0, 1 << 20) % (margin + 1)
    sizes = sizes.at[1:1 + 2 * couples:2].set(giver - shifted).at[2:2 + 2 * couples:2].set(taker + shifted)
    return sizes[jax.random.permutation(jax.random.fold_in(rng, 2), number_of)]


def scatter_about(stream_key, dims, spread, most, pieces=(), kind=jnp.bfloat16):
    values = spread * jax.random.normal(stream_key, dims, jnp.float32)
    if pieces:
        values = values * levels(stream_key, dims, pieces, -0.22, 0.18)
    return jnp.clip(values, -most, most).astype(kind)


def setup_inputs(seed: int = 0) -> dict:
    splits = jax.random.split(jax.random.key(seed), 7)
    queries = draw_queries(jax.random.fold_in(splits[6], 71), 0)
    keys_values = draw_keys_values(jax.random.fold_in(splits[6], 71), 0)
    out_weight = scatter_about(splits[2], (QUERY_HEADS * HEAD_SIZE, D), D ** -0.5, 0.125, ((0, 4),))
    cotangent = scatter_about(splits[3], (GROUPS, SEQUENCE_LENGTH, D), 1.0, 6.0, ((0, 4), (1, 8)))
    passage_lengths = jax.vmap(lambda own: ragged_sizes(own, LISTS, SEQUENCE_LENGTH - PREFIX, MOST, 2))(jax.random.split(splits[4], GROUPS)).reshape((GROUPS, LISTS)).astype(jnp.int32)
    causal_flags = place_ends(jax.random.randint(splits[5], (GROUPS, LISTS), 0, 2), jax.random.fold_in(splits[5], 1), 0, 1).astype(jnp.int32)
    return dict(queries=queries, keys_values=keys_values, out_weight=out_weight, cotangent=cotangent, passage_lengths=passage_lengths, causal_flags=causal_flags)


neg_fill = -1.0e30


def rounded(values):
    return lax.optimization_barrier(values.astype(jnp.bfloat16)).astype(jnp.float32)


def describe(lengths, causal, positions, prefix):
    lengths = lengths.astype(jnp.int32)
    starts = (prefix + jnp.cumsum(lengths) - lengths).astype(jnp.int32)
    segment_id = jnp.sum((starts[None, :] <= positions[:, None]).astype(jnp.int32), axis=1).astype(jnp.int32)
    labels = jnp.arange(1, lengths.shape[0] + 1, dtype=jnp.int32)
    flag_of = jnp.sum(jnp.where(segment_id[:, None] == labels[None, :], causal[None, :], 0), axis=1).astype(jnp.int32)
    flag_of = flag_of + (segment_id == 0).astype(jnp.int32)
    return segment_id, flag_of


def permitted(query_info, key_info, query_pos, key_pos):
    query_seg, query_flag = query_info
    key_seg, key_flag = key_info
    same_list = query_seg[:, None] == key_seg[None, :]
    visible = same_list | (key_seg[None, :] == 0)
    ordered = (key_pos[None, :] <= query_pos[:, None]) | ((query_flag[:, None] == 0) & same_list)
    return visible & ordered


def reference(queries, keys_values, out_weight, cotangent, passage_lengths, causal_flags):
    block_rows = SEQUENCE_LENGTH // N_BLK
    window = block_rows + 2 * MOST
    heads_per_group = QUERY_HEADS // KEY_VALUE_HEADS
    scale = HEAD_SIZE ** -0.5

    def one_group(operands):
        grouped_query, grouped_key_value, group_dy, lengths, causal = operands
        query_head_list = grouped_query.reshape(SEQUENCE_LENGTH, KEY_VALUE_HEADS, heads_per_group, HEAD_SIZE)
        key_value_head_list = grouped_key_value.reshape(SEQUENCE_LENGTH, KEY_VALUE_HEADS, 2 * HEAD_SIZE)
        attention_gradient = jnp.dot(group_dy, out_weight.T, preferred_element_type=jnp.float32).astype(jnp.bfloat16)
        head_gradients = attention_gradient.reshape(SEQUENCE_LENGTH, KEY_VALUE_HEADS, heads_per_group, HEAD_SIZE)

        def prepare(index):
            first_row = (index * block_rows).astype(jnp.int32)
            query_pos = first_row + jnp.arange(block_rows, dtype=jnp.int32)
            begin = jnp.clip(first_row - MOST, PREFIX, SEQUENCE_LENGTH - window).astype(jnp.int32)
            key_pos = jnp.concatenate([jnp.arange(PREFIX, dtype=jnp.int32), begin + jnp.arange(window, dtype=jnp.int32)])
            chosen = jnp.concatenate([key_value_head_list[:PREFIX], lax.dynamic_slice_in_dim(key_value_head_list, begin, window, 0)], axis=0)
            allowed = permitted(describe(lengths, causal, query_pos, PREFIX), describe(lengths, causal, key_pos, PREFIX), query_pos, key_pos)
            q_block = lax.dynamic_slice_in_dim(query_head_list, first_row, block_rows, 0).astype(jnp.float32)
            key_part = chosen[:, :, :HEAD_SIZE].astype(jnp.float32)
            value_part = chosen[:, :, HEAD_SIZE:].astype(jnp.float32)
            scores = jnp.einsum("qgrd,kgd->qgrk", q_block, key_part) * scale
            return first_row, begin, allowed[:, None, None, :], q_block, key_part, value_part, scores

        def forward(index):
            first_row, begin, allowed, q_block, key_part, value_part, scores = prepare(index)
            running_max = jnp.max(jnp.where(allowed, scores, neg_fill), axis=-1)
            totals = jnp.sum(jnp.where(allowed, jnp.exp(scores - running_max[..., None]), 0.0), axis=-1)
            log_norm = running_max + jnp.log(totals)
            probs = jnp.where(allowed, jnp.exp(scores - log_norm[..., None]), 0.0)
            result = jnp.einsum("qgrk,kgd->qgrd", rounded(probs), value_part).astype(jnp.bfloat16)
            return result, log_norm

        output_list, norm_values = lax.map(forward, jnp.arange(N_BLK, dtype=jnp.int32))
        attn = output_list.reshape(SEQUENCE_LENGTH, QUERY_HEADS * HEAD_SIZE)
        attention_per_head = output_list.reshape(SEQUENCE_LENGTH, KEY_VALUE_HEADS, heads_per_group, HEAD_SIZE)
        norm_total_rows = norm_values.reshape(SEQUENCE_LENGTH, KEY_VALUE_HEADS, heads_per_group)
        weight_gradient = jnp.dot(attn.T, group_dy, preferred_element_type=jnp.float32)

        def backward_pass(key_value_gradient, index):
            first_row, begin, allowed, q_block, key_part, value_part, scores = prepare(index)
            log_norm = lax.dynamic_slice_in_dim(norm_total_rows, first_row, block_rows, 0)
            probs = jnp.where(allowed, jnp.exp(scores - log_norm[..., None]), 0.0)
            out_block = lax.dynamic_slice_in_dim(attention_per_head, first_row, block_rows, 0).astype(jnp.float32)
            d_block = lax.dynamic_slice_in_dim(head_gradients, first_row, block_rows, 0).astype(jnp.float32)
            row_dot = jnp.sum(d_block * out_block, axis=-1)
            dprob = jnp.einsum("qgrd,kgd->qgrk", d_block, value_part)
            dscore = rounded(probs * (dprob - row_dot[..., None]))
            grad_q = (scale * jnp.einsum("qgrk,kgd->qgrd", dscore, key_part)).astype(jnp.bfloat16)
            grad_k = scale * jnp.einsum("qgrk,qgrd->kgd", dscore, q_block)
            grad_v = jnp.einsum("qgrk,qgrd->kgd", rounded(probs), d_block)
            both = jnp.concatenate([grad_k, grad_v], axis=-1)
            key_value_gradient = key_value_gradient.at[:PREFIX].add(both[:PREFIX])
            current = lax.dynamic_slice_in_dim(key_value_gradient, begin, window, 0)
            key_value_gradient = lax.dynamic_update_slice_in_dim(key_value_gradient, current + both[PREFIX:], begin, 0)
            return key_value_gradient, grad_q

        key_value_gradient, query_gradients = lax.scan(backward_pass, jnp.zeros((SEQUENCE_LENGTH, KEY_VALUE_HEADS, 2 * HEAD_SIZE), jnp.float32), jnp.arange(N_BLK, dtype=jnp.int32))
        return attn, query_gradients.reshape(SEQUENCE_LENGTH, QUERY_HEADS * HEAD_SIZE), key_value_gradient.reshape(SEQUENCE_LENGTH, KEY_VALUE_HEADS * 2 * HEAD_SIZE).astype(jnp.bfloat16), weight_gradient

    attn, grad_q, key_value_gradient, weight_gradient = lax.map(one_group, (queries, keys_values, cotangent, passage_lengths, causal_flags))
    return attn, grad_q, key_value_gradient, jnp.sum(weight_gradient, axis=0).astype(jnp.bfloat16)
```

```python
import functools

import jax
import jax.numpy as jnp
from jax import lax
from jax.experimental import pallas as pl
from jax.experimental.pallas import tpu as pltpu
from jax.sharding import PartitionSpec as P

neg_fill = -1e30


def passed_along(value, axis, steps):
    count = lax.axis_size(axis)
    pairs = [(source, (source + steps) % count) for source in range(count)]
    return lax.ppermute(value, axis, pairs)


def describe(lengths, causal, positions, prefix):
    starts = prefix + jnp.cumsum(lengths) - lengths
    segment_id = jnp.sum((starts[None, :] <= positions[:, None]).astype(jnp.int32), axis=1)
    labels = jnp.arange(1, lengths.shape[0] + 1, dtype=jnp.int32)
    flag_of = jnp.sum(jnp.where(segment_id[:, None] == labels[None, :], causal[None, :], 0), axis=1)
    flag_of = flag_of + (segment_id == 0).astype(jnp.int32)
    return (segment_id, flag_of)


def permitted(query_info, key_info, query_pos, key_pos):
    query_seg, query_flag = query_info
    key_seg, key_flag = key_info
    same_list = query_seg[:, None] == key_seg[None, :]
    visible = same_list | (key_seg[None, :] == 0)
    ordered = (key_pos[None, :] <= query_pos[:, None]) | (query_flag[:, None] == 0) & same_list
    return visible & ordered


def on_device(queries, keys_values, out_weight, cotangent, passage_lengths, causal_flags):
    q_rows, kv_rows = (
        lax.all_to_all(queries[0], "head", split_axis=1, concat_axis=0, tiled=True),
        lax.all_to_all(keys_values[0], "head", split_axis=1, concat_axis=0, tiled=True),
    )
    local_rows = q_rows.shape[0]
    cycle_size = lax.axis_size("blk")
    own_index = lax.axis_index("blk")
    seq_total = local_rows * cycle_size
    prefix = seq_total // 32
    head_dim = kv_rows.shape[1] // 2
    head_count = q_rows.shape[1] // head_dim
    flat_rows = local_rows * head_count
    scale = head_dim ** (-0.5)
    lengths = passage_lengths[0]
    causal = causal_flags[0]
    query_pos = own_index * local_rows + jnp.arange(local_rows, dtype=jnp.int32)
    query_info = describe(lengths, causal, query_pos, prefix)
    q_flat = q_rows.reshape(flat_rows, head_dim)

    def allowed_for(key_start, span_rows, floor_pos, live):
        key_pos = key_start + jnp.arange(span_rows, dtype=jnp.int32)
        allowed = permitted(
            query_info, describe(lengths, causal, key_pos, prefix), query_pos, key_pos
        )
        allowed = allowed & (key_pos >= floor_pos)[None, :] & live
        expanded = jnp.broadcast_to(
            allowed[:, None, :], (local_rows, head_count, span_rows)
        ).reshape(flat_rows, span_rows)
        return (allowed, expanded)

    def score_block(key_block):
        return (
            lax.dot_general(
                q_flat,
                key_block[:, :head_dim],
                (((1,), (1,)), ((), ())),
                preferred_element_type=jnp.float32,
            )
            * scale
        )

    def visit(state, key_block, key_start, floor_pos, live):
        allowed, expanded = allowed_for(key_start, key_block.shape[0], floor_pos, live)

        def visit_compute(inner):
            running_max, totals = inner
            scores = score_block(key_block)
            block_max = jnp.max(jnp.where(expanded, scores, neg_fill), axis=1)
            new_best = jnp.maximum(running_max, block_max)
            factor = jnp.exp(running_max - new_best)
            weights = jnp.where(expanded, jnp.exp(scores - new_best[:, None]), 0.0)
            totals = totals * factor + jnp.sum(weights, axis=1)
            return (new_best, totals)

        def visit_keep(inner):
            return inner

        return lax.cond(jnp.any(allowed), visit_compute, visit_keep, state)

    state_start = (
        jnp.full((flat_rows,), neg_fill, jnp.float32),
        jnp.zeros((flat_rows,), jnp.float32),
    )
    always = jnp.array(True)
    initial = (jnp.zeros((seq_total, 2 * head_dim), jnp.bfloat16),) + state_start
    shard_rows = lax.all_gather(kv_rows, "blk", axis=0, tiled=True)

    def one_block(index, inner):
        key_block = lax.dynamic_slice_in_dim(shard_rows, index * local_rows, local_rows, 0)
        return visit(inner, key_block, index * local_rows, 0, always)

    inner = lax.fori_loop(0, shard_rows.shape[0] // local_rows, one_block, tuple(initial[1:]))
    stored, running_max, totals = (shard_rows,) + tuple(inner)
    log_norm = running_max + jnp.log(totals)

    def stored_rows(key_start, span_rows):
        return lax.dynamic_slice_in_dim(stored, key_start, span_rows, 0)

    def add_values(accum, key_block, key_start, floor_pos, live):
        allowed, expanded = allowed_for(key_start, key_block.shape[0], floor_pos, live)

        def add_compute(acc_in):
            scores = score_block(key_block)
            probs = jnp.where(expanded, jnp.exp(scores - log_norm[:, None]), 0.0)
            return acc_in + jnp.dot(
                probs.astype(jnp.bfloat16),
                key_block[:, head_dim:],
                preferred_element_type=jnp.float32,
            )

        def add_keep(acc_in):
            return acc_in

        return lax.cond(jnp.any(allowed), add_compute, add_keep, accum)

    accum = jnp.zeros((flat_rows, head_dim), jnp.float32)

    def value_turn(index, acc_in):
        return add_values(
            acc_in, stored_rows(index * local_rows, local_rows), index * local_rows, 0, always
        )

    accum = lax.fori_loop(0, cycle_size, value_turn, accum)
    attn = accum.reshape(local_rows, head_count * head_dim).astype(jnp.bfloat16)
    project_shard_rows = lax.all_gather(cotangent[0], "head", axis=0, tiled=True)
    product = lax.dot_general(
        project_shard_rows, out_weight, (((1,), (1,)), ((), ())), preferred_element_type=jnp.float32
    )
    grads = product
    weight_acc = lax.dot_general(
        attn, project_shard_rows, (((0,), (0,)), ((), ())), preferred_element_type=jnp.float32
    )
    grads, weight_acc = (grads, weight_acc)
    attention_gradient = grads.astype(jnp.bfloat16)
    d_flat = attention_gradient.reshape(flat_rows, head_dim)
    row_dot = jnp.sum(
        (attention_gradient.astype(jnp.float32) * attn.astype(jnp.float32)).reshape(
            flat_rows, head_dim
        ),
        axis=1,
    )
    shares = lax.psum_scatter(
        weight_acc.astype(jnp.bfloat16), "blk", scatter_dimension=1, tiled=True
    ).astype(jnp.float32)
    shares = lax.psum(shares.astype(jnp.bfloat16), "dp")
    grad_weight = lax.all_gather(shares, "blk", axis=1, tiled=True)

    def contribute(grad_q, key_block, key_start, floor_pos, live):
        span_rows = key_block.shape[0]
        allowed, expanded = allowed_for(key_start, span_rows, floor_pos, live)

        def contribute_compute(grad_in):
            scores = score_block(key_block)
            probs = jnp.where(expanded, jnp.exp(scores - log_norm[:, None]), 0.0)
            dprob = lax.dot_general(
                d_flat,
                key_block[:, head_dim:],
                (((1,), (1,)), ((), ())),
                preferred_element_type=jnp.float32,
            )
            dscore = (probs * (dprob - row_dot[:, None])).astype(jnp.bfloat16)
            grad_out = grad_in + scale * jnp.dot(
                dscore, key_block[:, :head_dim], preferred_element_type=jnp.float32
            )
            grad_key = scale * lax.dot_general(
                dscore, q_flat, (((0,), (0,)), ((), ())), preferred_element_type=jnp.float32
            )
            grad_value = lax.dot_general(
                probs.astype(jnp.bfloat16),
                d_flat,
                (((0,), (0,)), ((), ())),
                preferred_element_type=jnp.float32,
            )
            return (grad_out, jnp.concatenate([grad_key, grad_value], axis=1))

        def skip(grad_in):
            return (grad_in, jnp.zeros((span_rows, 2 * head_dim), jnp.float32))

        return lax.cond(jnp.any(allowed), contribute_compute, skip, grad_q)

    grad_start = jnp.zeros((flat_rows, head_dim), jnp.float32)

    def turn_single(turn_index, state):
        grad_q, passing = state
        target = (own_index - 1 - turn_index) % cycle_size
        grad_q, piece_grad = contribute(
            grad_q, stored_rows(target * local_rows, local_rows), target * local_rows, 0, always
        )
        passing = passed_along((passing + piece_grad).astype(jnp.bfloat16), "blk", 1).astype(
            jnp.float32
        )
        return (grad_q, passing)

    zero_full = jnp.zeros((local_rows, 2 * head_dim), jnp.float32)
    grad_q, passing = lax.fori_loop(0, cycle_size - 1, turn_single, (grad_start, zero_full))
    grad_q, piece_grad = contribute(
        grad_q, stored_rows(own_index * local_rows, local_rows), own_index * local_rows, 0, always
    )
    key_value_gradient = passing + piece_grad
    grad_queries = grad_q.reshape(local_rows, head_count * head_dim).astype(jnp.bfloat16)
    return (
        attn[None],
        grad_queries[None],
        key_value_gradient.astype(jnp.bfloat16)[None],
        grad_weight,
    )


MESH = pl.DeviceIdType.MESH
f32, bf16 = jnp.float32, jnp.bfloat16
NN = (((1,), (0,)), ((), ()))
NT = (((1,), (1,)), ((), ()))


def mm(a, b, dims=NN):
    return lax.dot_general(a, b, dims, preferred_element_type=f32)


def fused_kernel(
    sizes,
    q_ref,
    kv_ref,
    w_ref,
    cot_ref,
    len_ref,
    flag_ref,
    attn_ref,
    gq_ref,
    gkv_ref,
    gw_ref,
    qg,
    kvl,
    edge,
    cotg,
    qt,
    ot,
    dt32,
    probs,
    dkv,
    back_out,
    back_in,
    wb,
    r0,
    r1,
    r2,
    qkv_send,
    qkv_recv,
    edge_send,
    edge_recv,
    cot_send,
    cot_recv,
    back_send,
    back_recv,
    red_send,
    red_recv,
):
    rows, most, prefix, hd, heads, chunks, units = sizes
    z, b, h = lax.axis_index("dp"), lax.axis_index("blk"), lax.axis_index("head")
    block = 4 * rows
    seq = 2 * block
    hc = heads * hd
    kvc = 2 * hd
    span = rows + 2 * most
    width = cot_ref.shape[1]
    cw = width // chunks
    uw = width // units
    h1 = h + 1 - 2 * lax.rem(h, 2)
    h2 = lax.rem(h + 2, 4)
    h3 = 3 - h
    peers = (h1, h2, h3)
    za = z + 1 - 2 * lax.rem(z, 2)
    zb = 3 - z
    bit_a = lax.rem((z + 1) // 2, 2)
    bit_b = z // 2
    partners = (((za, b, h), bit_a), ((zb, b, h), bit_b), ((z, 1 - b, h), b))

    barrier = pltpu.get_barrier_semaphore()
    others = [(z, b, p) for p in peers] + [(z, 1 - b, p) for p in (h, h1, h2, h3)]
    others += [(za, b, h), (zb, b, h)]
    for who in others:
        pl.semaphore_signal(barrier, inc=1, device_id=who, device_id_type=MESH)
    pl.semaphore_wait(barrier, len(others))

    def at(index, size):
        return pl.ds(pl.multiple_of(index * size, size), size)

    def remote(src, dst, send, recv, who):
        return pltpu.make_async_remote_copy(
            src_ref=src, dst_ref=dst, send_sem=send, recv_sem=recv,
            device_id=who, device_id_type=MESH,
        )

    kv_rows = pl.ds(pl.multiple_of(most + h * rows, most), rows)
    kv_copies, q_copies = [], []
    for i, p in ((1, h2), (2, h3), (0, h1)):
        kv_copies.append(remote(
            kv_ref.at[:, at(p, kvc)], kvl.at[kv_rows],
            qkv_send.at[i], qkv_recv.at[i], (z, b, p)))
        q_copies.append(remote(
            q_ref.at[:, at(p, hc)], qg.at[at(h, rows)],
            qkv_send.at[3 + i], qkv_recv.at[3 + i], (z, b, p)))

    def edge_copies(side):
        first = 0 if side == 0 else rows - most
        return [
            remote(
                kv_ref.at[pl.ds(first, most), at(p, kvc)], edge.at[side],
                edge_send.at[j], edge_recv.at[side], (z, 1 - b, p))
            for j, p in enumerate((h2, h3, h, h1))
        ]

    for c in kv_copies:
        c.start()
    for side, owner in ((0, 0), (1, 3)):
        @pl.when(h == owner)
        def _():
            for c in edge_copies(side):
                c.start()
    for c in q_copies:
        c.start()
    cot_far, cot_near, cot_relay = [], [], []
    for c in range(chunks):
        piece = cot_ref.at[:, pl.ds(c * cw, cw)]
        cot_far.append(remote(
            piece, cotg.at[c, at(h, rows)], cot_send.at[c], cot_recv.at[c], (z, b, h2)))
        cot_near.append(remote(
            piece, cotg.at[c, at(h, rows)], cot_send.at[chunks + c],
            cot_recv.at[chunks + c], (z, b, h1)))
        cot_relay.append(remote(
            cotg.at[c, at(h2, rows)], cotg.at[c, at(h2, rows)],
            cot_send.at[2 * chunks + c], cot_recv.at[2 * chunks + c], (z, b, h1)))
    for c in range(chunks):
        cot_far[c].start()
        cot_near[c].start()

    qg[at(h, rows), :] = q_ref[:, at(h, hc)]
    kvl[kv_rows, :] = kv_ref[:, at(h, kvc)]
    for c in range(chunks):
        cotg[c, at(h, rows), :] = cot_ref[:, c * cw : (c + 1) * cw]
    dkv[...] = jnp.zeros_like(dkv)

    lists = len_ref.shape[1]
    len_row = len_ref[...].astype(f32)
    flag_row = flag_ref[...].astype(f32)
    ii = lax.broadcasted_iota(jnp.int32, (lists, lists), 0)
    jj = lax.broadcasted_iota(jnp.int32, (lists, lists), 1)
    len_col = jnp.sum(jnp.where(ii == jj, len_row, 0.0), axis=1, keepdims=True)
    flag_col = jnp.sum(jnp.where(ii == jj, flag_row, 0.0), axis=1, keepdims=True)
    start_col = prefix + jnp.sum(jnp.where(jj < ii, len_row, 0.0), axis=1, keepdims=True)
    start_row = prefix + jnp.sum(jnp.where(ii < jj, len_col, 0.0), axis=0, keepdims=True)
    base = (b * block).astype(f32)
    key_total = block + 2 * most
    kpos = lax.broadcasted_iota(jnp.int32, (key_total, 1), 0).astype(f32) + (base - most)
    kseg = jnp.sum(jnp.where(start_row <= kpos, 1.0, 0.0), axis=1, keepdims=True)
    kseg = jnp.where((kpos < prefix) | (kpos >= seq), -1.0, kseg)
    ppos = lax.broadcasted_iota(jnp.int32, (prefix, 1), 0).astype(f32)
    pseg = jnp.zeros((prefix, 1), f32)
    qpos = lax.broadcasted_iota(jnp.int32, (1, block), 1).astype(f32) + base
    qseg = jnp.sum(jnp.where(start_col <= qpos, 1.0, 0.0), axis=0, keepdims=True)
    label = lax.broadcasted_iota(jnp.int32, (lists, 1), 0).astype(f32) + 1.0
    qflag = jnp.sum(jnp.where(label == qseg, flag_col, 0.0), axis=0, keepdims=True)
    qflag = qflag + jnp.where(qseg == 0.0, 1.0, 0.0)

    for c in kv_copies:
        c.wait_recv()
    for side in range(2):
        edge_copies(side)[0].wait_recv()
    first = jnp.where(b == 0, kvl[most : most + prefix, :], edge[0, :prefix, :])
    kvl[:most, :] = jnp.where(b == 0, jnp.zeros_like(edge[1]), edge[1])
    kvl[most + block :, :] = jnp.where(b == 0, edge[0], jnp.zeros_like(edge[0]))
    for c in q_copies:
        c.wait_recv()
    qt[...] = (qg[...].astype(f32) * (hd ** -0.5)).T.astype(bf16)
    blank = jnp.zeros((hd, heads * rows), bf16)

    def lanes(ref, tile):
        return jnp.concatenate(
            [ref[i * hd : (i + 1) * hd, tile * rows : (tile + 1) * rows] for i in range(heads)],
            axis=1,
        )

    def stacked(value):
        return jnp.concatenate(
            [value[:, i * rows : (i + 1) * rows] for i in range(heads)], axis=0
        )

    def window(tile):
        return jnp.concatenate([kvl[tile * rows : tile * rows + span, :], first], axis=0)

    def forward(tile):
        kw = window(tile)
        scores = mm(kw, jnp.concatenate([lanes(qt, tile), blank], axis=0))
        cut = slice(tile * rows, tile * rows + span)
        kp = jnp.concatenate([kpos[cut], ppos], axis=0)
        ks = jnp.concatenate([kseg[cut], pseg], axis=0)
        sl = slice(tile * rows, (tile + 1) * rows)
        qp, qs, qf = qpos[:, sl], qseg[:, sl], qflag[:, sl]
        same = ks == qs
        allowed = (same | (ks == 0.0)) & ((kp <= qp) | ((qf == 0.0) & same))
        fill = jnp.where(allowed, 0.0, neg_fill)
        scores = scores + jnp.concatenate([fill] * heads, axis=1)
        best = jnp.max(scores, axis=0, keepdims=True)
        e = jnp.exp(scores - best)
        p = e * (1.0 / jnp.sum(e, axis=0, keepdims=True))
        probs[tile] = p
        out = stacked(mm(kw.T[hd:], p.astype(bf16)))
        ot[:, sl] = out.astype(bf16)
        attn_ref[sl, :] = out.T.astype(bf16)

    def backward(tile):
        kw = window(tile)
        sl = slice(tile * rows, (tile + 1) * rows)
        p = probs[tile]
        d = lanes(dt32, tile).astype(bf16)
        o = lanes(ot, tile)
        row_dot = jnp.sum(d.astype(f32) * o.astype(f32), axis=0, keepdims=True)
        d_pad = jnp.concatenate([blank, d], axis=0)
        q_pad = jnp.concatenate([lanes(qt, tile), blank], axis=0)
        ds = (p * (mm(kw, d_pad) - row_dot)).astype(bf16)
        gq = stacked(mm(kw.T[:hd], ds)) * (hd ** -0.5)
        gq_ref[sl, :] = gq.T.astype(bf16)
        both = mm(ds, q_pad, NT) + mm(p.astype(bf16), d_pad, NT)
        cut = slice(tile * rows, tile * rows + span)
        dkv[cut, :] += both[:span]
        tail = slice(key_total, key_total + prefix)
        dkv[tail, :] += both[span:]

    def reduce_copy(u, k):
        dims = [partners[(u + i) % 3] for i in range(3)]
        size = hc
        keep = []
        low = 0
        for _, bit in dims:
            size = size // 2
            low = low + bit * size
            keep.append((low, size))
        sems = (red_send.at[u * 6 + k], red_recv.at[u * 6 + k])
        if k < 3:
            who, bit = dims[k]
            low, size = keep[k]
            away = low + (1 - 2 * bit) * size
            src = wb.at[u, pl.ds(pl.multiple_of(away, size), size)]
            return remote(src, (r0, r1, r2)[k].at[u], *sems, who)
        low, size = keep[5 - k]
        part = gw_ref.at[pl.ds(pl.multiple_of(low, size), size), pl.ds(u * uw, uw)]
        return remote(part, part, *sems, dims[5 - k][0])

    def reduce_step(u, k):
        if k > 0:
            reduce_copy(u, k - 1).wait_recv()
        if 0 < k < 4:
            dims = [partners[(u + i) % 3] for i in range(3)]
            low, size = 0, hc
            for _, bit in dims[:k]:
                size = size // 2
                low = low + bit * size
            at_rows = pl.ds(pl.multiple_of(low, size), size)
            total = wb[u, at_rows, :].astype(f32) + (r0, r1, r2)[k - 1][u].astype(f32)
            if k < 3:
                wb[u, at_rows, :] = total.astype(bf16)
            else:
                gw_ref[at_rows, u * uw : (u + 1) * uw] = total.astype(bf16)
        if k < 6:
            reduce_copy(u, k).start()

    progress = [-1] * units

    def advance(limit):
        for u in range(limit):
            if progress[u] < 6:
                progress[u] += 1
                reduce_step(u, progress[u])

    per = units // chunks
    for tile in range(4):
        forward(tile)
    for c in range(chunks):
        cot_far[c].wait_recv()
        cot_relay[c].start()
        cot_near[c].wait_recv()
        advance(c * per)
        cot_relay[c].wait_recv()
        whole = cotg[c]
        grad = mm(ot[...], whole).astype(bf16)
        for i in range(per):
            wb[c * per + i] = grad[:, i * uw : (i + 1) * uw]
        for i in range(per):
            progress[c * per + i] = 0
            reduce_step(c * per + i, 0)
        part = mm(w_ref[:, c * cw : (c + 1) * cw], whole, NT)
        if c == 0:
            dt32[...] = part
        else:
            dt32[...] += part
    for tile in range(4):
        advance(units)
        backward(tile)
    zero_pre = jnp.zeros((most - prefix, kvc), f32)
    pre = dkv[key_total : key_total + prefix, :]
    pre_full = jnp.concatenate([pre, zero_pre], axis=0)
    back_out[0] = jnp.where(b == 0, dkv[most + block : key_total, :], pre_full)
    back_out[1] = dkv[:most, :]
    backs = [
        remote(back_out.at[i], back_in.at[i], back_send.at[i], back_recv.at[i], (z, 1 - b, h))
        for i in range(2)
    ]
    for c in backs:
        c.start()
    advance(units)
    for c in backs:
        c.wait_recv()
    head_part = dkv[most : 2 * most, :] + back_in[0] + jnp.where(b == 0, pre_full, 0.0)
    gkv_ref[:most, :] = head_part.astype(bf16)
    gkv_ref[most : block - most, :] = dkv[2 * most : block, :].astype(bf16)
    gkv_ref[block - most :, :] = (dkv[block : block + most, :] + back_in[1]).astype(bf16)
    while min(progress) < 6:
        advance(units)
    for c in kv_copies + q_copies + cot_far + cot_near + cot_relay + backs:
        c.wait_send()
    for side, owner in ((0, 0), (1, 3)):
        @pl.when(h == owner)
        def _():
            for c in edge_copies(side):
                c.wait_send()
    for u in range(units):
        for k in range(6):
            reduce_copy(u, k).wait_send()


def on_device_fused(queries, keys_values, out_weight, cotangent, passage_lengths, causal_flags):
    chunks, units = 4, 8
    rows = queries.shape[1]
    block = 4 * rows
    seq = 2 * block
    most, prefix = seq // 16, seq // 32
    kvc = keys_values.shape[2] // 4
    hc = queries.shape[2] // 4
    hd = kvc // 2
    heads = hc // hd
    width = cotangent.shape[2]
    key_total = block + 2 * most
    window = rows + 2 * most + prefix
    vmem = pl.BlockSpec(memory_space=pltpu.VMEM)
    uw = width // units
    sem = pltpu.SemaphoreType.DMA
    attn, gq, gkv, gw = pl.pallas_call(
        functools.partial(fused_kernel, (rows, most, prefix, hd, heads, chunks, units)),
        out_shape=(
            jax.ShapeDtypeStruct((block, hc), bf16),
            jax.ShapeDtypeStruct((block, hc), bf16),
            jax.ShapeDtypeStruct((block, kvc), bf16),
            jax.ShapeDtypeStruct((hc, width), bf16),
        ),
        in_specs=[vmem] * 6,
        out_specs=(vmem,) * 4,
        scratch_shapes=[
            pltpu.VMEM((block, hc), bf16),
            pltpu.VMEM((key_total, kvc), bf16),
            pltpu.VMEM((2, most, kvc), bf16),
            pltpu.VMEM((chunks, block, width // chunks), bf16),
            pltpu.VMEM((hc, block), bf16),
            pltpu.VMEM((hc, block), bf16),
            pltpu.VMEM((hc, block), f32),
            pltpu.VMEM((4, window, heads * rows), f32),
            pltpu.VMEM((key_total + prefix, kvc), f32),
            pltpu.VMEM((2, most, kvc), f32),
            pltpu.VMEM((2, most, kvc), f32),
            pltpu.VMEM((units, hc, uw), bf16),
            pltpu.VMEM((units, hc // 2, uw), bf16),
            pltpu.VMEM((units, hc // 4, uw), bf16),
            pltpu.VMEM((units, hc // 8, uw), bf16),
            sem((6,)),
            sem((6,)),
            sem((4,)),
            sem((2,)),
            sem((3 * chunks,)),
            sem((3 * chunks,)),
            sem((2,)),
            sem((2,)),
            sem((units * 6,)),
            sem((units * 6,)),
        ],
        compiler_params=pltpu.CompilerParams(
            collective_id=0, has_side_effects=True, vmem_limit_bytes=48 * 1024 * 1024
        ),
    )(
        queries[0], keys_values[0], out_weight, cotangent[0], passage_lengths, causal_flags
    )
    return attn[None], gq[None], gkv[None], gw


def fits(mesh):
    sizes = (mesh.shape["dp"], mesh.shape["blk"], mesh.shape["head"])
    return sizes == (4, 2, 4)


def solution(mesh):
    return jax.shard_map(
        on_device_fused if fits(mesh) else on_device,
        mesh=mesh,
        in_specs=(
            P("dp", ("blk", "head"), None),
            P("dp", ("blk", "head"), None),
            P("head", None),
            P("dp", ("blk", "head"), None),
            P("dp", None),
            P("dp", None),
        ),
        out_specs=(
            P("dp", "blk", "head"),
            P("dp", "blk", "head"),
            P("dp", "blk", "head"),
            P("head", None),
        ),
        check_vma=False,
    )
```

```python
import functools

import jax
import jax.numpy as jnp
from jax import lax
from jax.experimental import pallas as pl
from jax.experimental.pallas import tpu as pltpu
from jax.sharding import PartitionSpec as P

neg_fill = -1e30


def passed_along(value, axis, steps):
    count = lax.axis_size(axis)
    pairs = [(source, (source + steps) % count) for source in range(count)]
    return lax.ppermute(value, axis, pairs)


def describe(lengths, causal, positions, prefix):
    starts = prefix + jnp.cumsum(lengths) - lengths
    segment_id = jnp.sum((starts[None, :] <= positions[:, None]).astype(jnp.int32), axis=1)
    labels = jnp.arange(1, lengths.shape[0] + 1, dtype=jnp.int32)
    flag_of = jnp.sum(jnp.where(segment_id[:, None] == labels[None, :], causal[None, :], 0), axis=1)
    flag_of = flag_of + (segment_id == 0).astype(jnp.int32)
    return (segment_id, flag_of)


def permitted(query_info, key_info, query_pos, key_pos):
    query_seg, query_flag = query_info
    key_seg, key_flag = key_info
    same_list = query_seg[:, None] == key_seg[None, :]
    visible = same_list | (key_seg[None, :] == 0)
    ordered = (key_pos[None, :] <= query_pos[:, None]) | (query_flag[:, None] == 0) & same_list
    return visible & ordered


def on_device(queries, keys_values, out_weight, cotangent, passage_lengths, causal_flags):
    q_rows, kv_rows = (
        lax.all_to_all(queries[0], "head", split_axis=1, concat_axis=0, tiled=True),
        lax.all_to_all(keys_values[0], "head", split_axis=1, concat_axis=0, tiled=True),
    )
    local_rows = q_rows.shape[0]
    cycle_size = lax.axis_size("blk")
    own_index = lax.axis_index("blk")
    seq_total = local_rows * cycle_size
    prefix = seq_total // 32
    head_dim = kv_rows.shape[1] // 2
    head_count = q_rows.shape[1] // head_dim
    flat_rows = local_rows * head_count
    scale = head_dim ** (-0.5)
    lengths = passage_lengths[0]
    causal = causal_flags[0]
    query_pos = own_index * local_rows + jnp.arange(local_rows, dtype=jnp.int32)
    query_info = describe(lengths, causal, query_pos, prefix)
    q_flat = q_rows.reshape(flat_rows, head_dim)

    def allowed_for(key_start, span_rows, floor_pos, live):
        key_pos = key_start + jnp.arange(span_rows, dtype=jnp.int32)
        allowed = permitted(
            query_info, describe(lengths, causal, key_pos, prefix), query_pos, key_pos
        )
        allowed = allowed & (key_pos >= floor_pos)[None, :] & live
        expanded = jnp.broadcast_to(
            allowed[:, None, :], (local_rows, head_count, span_rows)
        ).reshape(flat_rows, span_rows)
        return (allowed, expanded)

    def score_block(key_block):
        return (
            lax.dot_general(
                q_flat,
                key_block[:, :head_dim],
                (((1,), (1,)), ((), ())),
                preferred_element_type=jnp.float32,
            )
            * scale
        )

    def visit(state, key_block, key_start, floor_pos, live):
        allowed, expanded = allowed_for(key_start, key_block.shape[0], floor_pos, live)

        def visit_compute(inner):
            running_max, totals = inner
            scores = score_block(key_block)
            block_max = jnp.max(jnp.where(expanded, scores, neg_fill), axis=1)
            new_best = jnp.maximum(running_max, block_max)
            factor = jnp.exp(running_max - new_best)
            weights = jnp.where(expanded, jnp.exp(scores - new_best[:, None]), 0.0)
            totals = totals * factor + jnp.sum(weights, axis=1)
            return (new_best, totals)

        def visit_keep(inner):
            return inner

        return lax.cond(jnp.any(allowed), visit_compute, visit_keep, state)

    state_start = (
        jnp.full((flat_rows,), neg_fill, jnp.float32),
        jnp.zeros((flat_rows,), jnp.float32),
    )
    always = jnp.array(True)
    initial = (jnp.zeros((seq_total, 2 * head_dim), jnp.bfloat16),) + state_start
    shard_rows = lax.all_gather(kv_rows, "blk", axis=0, tiled=True)

    def one_block(index, inner):
        key_block = lax.dynamic_slice_in_dim(shard_rows, index * local_rows, local_rows, 0)
        return visit(inner, key_block, index * local_rows, 0, always)

    inner = lax.fori_loop(0, shard_rows.shape[0] // local_rows, one_block, tuple(initial[1:]))
    stored, running_max, totals = (shard_rows,) + tuple(inner)
    log_norm = running_max + jnp.log(totals)

    def stored_rows(key_start, span_rows):
        return lax.dynamic_slice_in_dim(stored, key_start, span_rows, 0)

    def add_values(accum, key_block, key_start, floor_pos, live):
        allowed, expanded = allowed_for(key_start, key_block.shape[0], floor_pos, live)

        def add_compute(acc_in):
            scores = score_block(key_block)
            probs = jnp.where(expanded, jnp.exp(scores - log_norm[:, None]), 0.0)
            return acc_in + jnp.dot(
                probs.astype(jnp.bfloat16),
                key_block[:, head_dim:],
                preferred_element_type=jnp.float32,
            )

        def add_keep(acc_in):
            return acc_in

        return lax.cond(jnp.any(allowed), add_compute, add_keep, accum)

    accum = jnp.zeros((flat_rows, head_dim), jnp.float32)

    def value_turn(index, acc_in):
        return add_values(
            acc_in, stored_rows(index * local_rows, local_rows), index * local_rows, 0, always
        )

    accum = lax.fori_loop(0, cycle_size, value_turn, accum)
    attn = accum.reshape(local_rows, head_count * head_dim).astype(jnp.bfloat16)
    project_shard_rows = lax.all_gather(cotangent[0], "head", axis=0, tiled=True)
    product = lax.dot_general(
        project_shard_rows, out_weight, (((1,), (1,)), ((), ())), preferred_element_type=jnp.float32
    )
    grads = product
    weight_acc = lax.dot_general(
        attn, project_shard_rows, (((0,), (0,)), ((), ())), preferred_element_type=jnp.float32
    )
    grads, weight_acc = (grads, weight_acc)
    attention_gradient = grads.astype(jnp.bfloat16)
    d_flat = attention_gradient.reshape(flat_rows, head_dim)
    row_dot = jnp.sum(
        (attention_gradient.astype(jnp.float32) * attn.astype(jnp.float32)).reshape(
            flat_rows, head_dim
        ),
        axis=1,
    )
    shares = lax.psum_scatter(
        weight_acc.astype(jnp.bfloat16), "blk", scatter_dimension=1, tiled=True
    ).astype(jnp.float32)
    shares = lax.psum(shares.astype(jnp.bfloat16), "dp")
    grad_weight = lax.all_gather(shares, "blk", axis=1, tiled=True)

    def contribute(grad_q, key_block, key_start, floor_pos, live):
        span_rows = key_block.shape[0]
        allowed, expanded = allowed_for(key_start, span_rows, floor_pos, live)

        def contribute_compute(grad_in):
            scores = score_block(key_block)
            probs = jnp.where(expanded, jnp.exp(scores - log_norm[:, None]), 0.0)
            dprob = lax.dot_general(
                d_flat,
                key_block[:, head_dim:],
                (((1,), (1,)), ((), ())),
                preferred_element_type=jnp.float32,
            )
            dscore = (probs * (dprob - row_dot[:, None])).astype(jnp.bfloat16)
            grad_out = grad_in + scale * jnp.dot(
                dscore, key_block[:, :head_dim], preferred_element_type=jnp.float32
            )
            grad_key = scale * lax.dot_general(
                dscore, q_flat, (((0,), (0,)), ((), ())), preferred_element_type=jnp.float32
            )
            grad_value = lax.dot_general(
                probs.astype(jnp.bfloat16),
                d_flat,
                (((0,), (0,)), ((), ())),
                preferred_element_type=jnp.float32,
            )
            return (grad_out, jnp.concatenate([grad_key, grad_value], axis=1))

        def skip(grad_in):
            return (grad_in, jnp.zeros((span_rows, 2 * head_dim), jnp.float32))

        return lax.cond(jnp.any(allowed), contribute_compute, skip, grad_q)

    grad_start = jnp.zeros((flat_rows, head_dim), jnp.float32)

    def turn_single(turn_index, state):
        grad_q, passing = state
        target = (own_index - 1 - turn_index) % cycle_size
        grad_q, piece_grad = contribute(
            grad_q, stored_rows(target * local_rows, local_rows), target * local_rows, 0, always
        )
        passing = passed_along((passing + piece_grad).astype(jnp.bfloat16), "blk", 1).astype(
            jnp.float32
        )
        return (grad_q, passing)

    zero_full = jnp.zeros((local_rows, 2 * head_dim), jnp.float32)
    grad_q, passing = lax.fori_loop(0, cycle_size - 1, turn_single, (grad_start, zero_full))
    grad_q, piece_grad = contribute(
        grad_q, stored_rows(own_index * local_rows, local_rows), own_index * local_rows, 0, always
    )
    key_value_gradient = passing + piece_grad
    grad_queries = grad_q.reshape(local_rows, head_count * head_dim).astype(jnp.bfloat16)
    return (
        attn[None],
        grad_queries[None],
        key_value_gradient.astype(jnp.bfloat16)[None],
        grad_weight,
    )


MESH = pl.DeviceIdType.MESH
f32, bf16 = jnp.float32, jnp.bfloat16
NN = (((1,), (0,)), ((), ()))
NT = (((1,), (1,)), ((), ()))


def mm(a, b, dims=NN):
    return lax.dot_general(a, b, dims, preferred_element_type=f32)


def fused_kernel(
    sizes,
    q_hbm,
    kv_hbm,
    w_hbm,
    cot_hbm,
    len_ref,
    flag_ref,
    attn_ref,
    gq_ref,
    gkv_ref,
    gw_ref,
    q_ref,
    kv_ref,
    w_ref,
    local_sem,
    qg,
    kvl,
    edge,
    cotg,
    qt,
    ot,
    dt32,
    probs,
    dkv,
    back_out,
    back_in,
    wb,
    r0,
    r1,
    r2,
    qkv_send,
    qkv_recv,
    edge_send,
    edge_recv,
    cot_send,
    cot_recv,
    back_send,
    back_recv,
    red_send,
    red_recv,
):
    rows, most, prefix, hd, heads, chunks, units = sizes
    z, b, h = lax.axis_index("dp"), lax.axis_index("blk"), lax.axis_index("head")
    block = 4 * rows
    seq = 2 * block
    hc = heads * hd
    kvc = 2 * hd
    span = rows + 2 * most
    width = cot_hbm.shape[1]
    cw = width // chunks
    uw = width // units
    h1 = h + 1 - 2 * lax.rem(h, 2)
    h2 = lax.rem(h + 2, 4)
    h3 = 3 - h
    peers = (h1, h2, h3)
    za = z + 1 - 2 * lax.rem(z, 2)
    zb = lax.rem(z + 2, 4)
    bit_a = lax.rem(z, 2)
    bit_b = z // 2
    partners = (((za, b, h), bit_a), ((zb, b, h), bit_b), ((z, 1 - b, h), b))

    barrier = pltpu.get_barrier_semaphore()
    others = [(z, b, p) for p in peers] + [(z, 1 - b, p) for p in (h, h1, h2, h3)]
    others += [(za, b, h), (zb, b, h)]
    for who in others:
        pl.semaphore_signal(barrier, inc=1, device_id=who, device_id_type=MESH)

    def at(index, size):
        return pl.ds(pl.multiple_of(index * size, size), size)

    def remote(src, dst, send, recv, who):
        return pltpu.make_async_remote_copy(
            src_ref=src, dst_ref=dst, send_sem=send, recv_sem=recv,
            device_id=who, device_id_type=MESH,
        )

    loads = [
        pltpu.make_async_copy(kv_hbm, kv_ref, local_sem.at[0]),
        pltpu.make_async_copy(q_hbm, q_ref, local_sem.at[1]),
    ]
    for c in range(chunks):
        loads.append(pltpu.make_async_copy(
            cot_hbm.at[:, pl.ds(c * cw, cw)], cotg.at[c, at(h, rows)], local_sem.at[3 + c]))
    loads.append(pltpu.make_async_copy(w_hbm, w_ref, local_sem.at[2]))
    for c in loads:
        c.start()
    pl.semaphore_wait(barrier, len(others))

    kv_rows = pl.ds(pl.multiple_of(most + h * rows, most), rows)
    kv_copies, q_copies = [], []
    for i, p in ((1, h2), (2, h3), (0, h1)):
        kv_copies.append(remote(
            kv_ref.at[:, at(p, kvc)], kvl.at[kv_rows],
            qkv_send.at[i], qkv_recv.at[i], (z, b, p)))
        q_copies.append(remote(
            q_ref.at[:, at(p, hc)], qg.at[at(h, rows)],
            qkv_send.at[3 + i], qkv_recv.at[3 + i], (z, b, p)))

    def edge_copies(side):
        first = 0 if side == 0 else rows - most
        return [
            remote(
                kv_ref.at[pl.ds(first, most), at(p, kvc)], edge.at[side],
                edge_send.at[j], edge_recv.at[side], (z, 1 - b, p))
            for j, p in enumerate((h2, h3, h, h1))
        ]

    loads[0].wait()
    for c in kv_copies:
        c.start()
    for side, owner in ((0, 0), (1, 3)):
        @pl.when(h == owner)
        def _():
            for c in edge_copies(side):
                c.start()
    loads[1].wait()
    for c in q_copies:
        c.start()
    cot_far, cot_near, cot_relay = [], [], []
    for c in range(chunks):
        piece = cotg.at[c, at(h, rows)]
        cot_far.append(remote(
            piece, cotg.at[c, at(h, rows)], cot_send.at[c], cot_recv.at[c], (z, b, h2)))
        cot_near.append(remote(
            piece, cotg.at[c, at(h, rows)], cot_send.at[chunks + c],
            cot_recv.at[chunks + c], (z, b, h1)))
        cot_relay.append(remote(
            cotg.at[c, at(h2, rows)], cotg.at[c, at(h2, rows)],
            cot_send.at[2 * chunks + c], cot_recv.at[2 * chunks + c], (z, b, h1)))
    for c in range(chunks):
        loads[2 + c].wait()
        cot_far[c].start()
        cot_near[c].start()

    qg[at(h, rows), :] = q_ref[:, at(h, hc)]
    kvl[kv_rows, :] = kv_ref[:, at(h, kvc)]
    dkv[...] = jnp.zeros_like(dkv)

    lists = len_ref.shape[1]
    len_row = len_ref[...].astype(f32)
    flag_row = flag_ref[...].astype(f32)
    ii = lax.broadcasted_iota(jnp.int32, (lists, lists), 0)
    jj = lax.broadcasted_iota(jnp.int32, (lists, lists), 1)
    len_col = jnp.sum(jnp.where(ii == jj, len_row, 0.0), axis=1, keepdims=True)
    flag_col = jnp.sum(jnp.where(ii == jj, flag_row, 0.0), axis=1, keepdims=True)
    start_col = prefix + jnp.sum(jnp.where(jj < ii, len_row, 0.0), axis=1, keepdims=True)
    start_row = prefix + jnp.sum(jnp.where(ii < jj, len_col, 0.0), axis=0, keepdims=True)
    base = (b * block).astype(f32)
    key_total = block + 2 * most
    kpos = lax.broadcasted_iota(jnp.int32, (key_total, 1), 0).astype(f32) + (base - most)
    kseg = jnp.sum(jnp.where(start_row <= kpos, 1.0, 0.0), axis=1, keepdims=True)
    kseg = jnp.where((kpos < prefix) | (kpos >= seq), -1.0, kseg)
    ppos = lax.broadcasted_iota(jnp.int32, (prefix, 1), 0).astype(f32)
    pseg = jnp.zeros((prefix, 1), f32)
    qpos = lax.broadcasted_iota(jnp.int32, (1, block), 1).astype(f32) + base
    qseg = jnp.sum(jnp.where(start_col <= qpos, 1.0, 0.0), axis=0, keepdims=True)
    label = lax.broadcasted_iota(jnp.int32, (lists, 1), 0).astype(f32) + 1.0
    qflag = jnp.sum(jnp.where(label == qseg, flag_col, 0.0), axis=0, keepdims=True)
    qflag = qflag + jnp.where(qseg == 0.0, 1.0, 0.0)

    for c in kv_copies:
        c.wait_recv()
    for side in range(2):
        edge_copies(side)[0].wait_recv()
    first = jnp.where(b == 0, kvl[most : most + prefix, :], edge[0, :prefix, :])
    kvl[:most, :] = jnp.where(b == 0, jnp.zeros_like(edge[1]), edge[1])
    kvl[most + block :, :] = jnp.where(b == 0, edge[0], jnp.zeros_like(edge[0]))
    for c in q_copies:
        c.wait_recv()
    qt[...] = (qg[...].astype(f32) * (hd ** -0.5)).T.astype(bf16)
    blank = jnp.zeros((hd, heads * rows), bf16)

    def lanes(ref, tile):
        return jnp.concatenate(
            [ref[i * hd : (i + 1) * hd, tile * rows : (tile + 1) * rows] for i in range(heads)],
            axis=1,
        )

    def stacked(value):
        return jnp.concatenate(
            [value[:, i * rows : (i + 1) * rows] for i in range(heads)], axis=0
        )

    def window(tile):
        return jnp.concatenate([kvl[tile * rows : tile * rows + span, :], first], axis=0)

    def forward(tile):
        kw = window(tile)
        scores = mm(kw, jnp.concatenate([lanes(qt, tile), blank], axis=0))
        cut = slice(tile * rows, tile * rows + span)
        kp = jnp.concatenate([kpos[cut], ppos], axis=0)
        ks = jnp.concatenate([kseg[cut], pseg], axis=0)
        sl = slice(tile * rows, (tile + 1) * rows)
        qp, qs, qf = qpos[:, sl], qseg[:, sl], qflag[:, sl]
        same = ks == qs
        allowed = (same | (ks == 0.0)) & ((kp <= qp) | ((qf == 0.0) & same))
        fill = jnp.where(allowed, 0.0, neg_fill)
        scores = scores + jnp.concatenate([fill] * heads, axis=1)
        best = jnp.max(scores, axis=0, keepdims=True)
        e = jnp.exp(scores - best)
        p = e * (1.0 / jnp.sum(e, axis=0, keepdims=True))
        probs[tile] = p
        out = stacked(mm(kw.T[hd:], p.astype(bf16)))
        ot[:, sl] = out.astype(bf16)
        attn_ref[sl, :] = out.T.astype(bf16)

    def backward(tile):
        kw = window(tile)
        sl = slice(tile * rows, (tile + 1) * rows)
        p = probs[tile]
        d = lanes(dt32, tile).astype(bf16)
        o = lanes(ot, tile)
        row_dot = jnp.sum(d.astype(f32) * o.astype(f32), axis=0, keepdims=True)
        d_pad = jnp.concatenate([blank, d], axis=0)
        q_pad = jnp.concatenate([lanes(qt, tile), blank], axis=0)
        ds = (p * (mm(kw, d_pad) - row_dot)).astype(bf16)
        gq = stacked(mm(kw.T[:hd], ds)) * (hd ** -0.5)
        gq_ref[sl, :] = gq.T.astype(bf16)
        both = mm(ds, q_pad, NT) + mm(p.astype(bf16), d_pad, NT)
        cut = slice(tile * rows, tile * rows + span)
        dkv[cut, :] += both[:span]
        tail = slice(key_total, key_total + prefix)
        dkv[tail, :] += both[span:]

    def order(u):
        near, far, side = partners
        return (near, side, far) if u % 3 == 1 else (side, near, far)

    def reduce_copy(u, k):
        dims = order(u)
        size = hc
        keep = []
        low = 0
        for _, bit in dims:
            size = size // 2
            low = low + bit * size
            keep.append((low, size))
        sems = (red_send.at[u * 6 + k], red_recv.at[u * 6 + k])
        if k < 3:
            who, bit = dims[k]
            low, size = keep[k]
            away = low + (1 - 2 * bit) * size
            src = wb.at[u, pl.ds(pl.multiple_of(away, size), size)]
            return remote(src, (r0, r1, r2)[k].at[u], *sems, who)
        low, size = keep[5 - k]
        part = gw_ref.at[pl.ds(pl.multiple_of(low, size), size), pl.ds(u * uw, uw)]
        return remote(part, part, *sems, dims[5 - k][0])

    def reduce_step(u, k):
        if k > 0:
            reduce_copy(u, k - 1).wait_recv()
        if 0 < k < 4:
            dims = order(u)
            low, size = 0, hc
            for _, bit in dims[:k]:
                size = size // 2
                low = low + bit * size
            at_rows = pl.ds(pl.multiple_of(low, size), size)
            total = wb[u, at_rows, :].astype(f32) + (r0, r1, r2)[k - 1][u].astype(f32)
            if k < 3:
                wb[u, at_rows, :] = total.astype(bf16)
            else:
                gw_ref[at_rows, u * uw : (u + 1) * uw] = total.astype(bf16)
        if k < 6:
            reduce_copy(u, k).start()

    progress = [-1] * units

    def advance(turn):
        for u in range(units):
            if 0 <= progress[u] < 6 and (turn - u) % 2 == 0:
                progress[u] += 1
                reduce_step(u, progress[u])

    loads[2 + chunks].wait()
    per = units // chunks
    for tile in range(4):
        with jax.named_scope(f'fwd{tile}'):
            forward(tile)
    for c in range(chunks):
        cot_far[c].wait_recv()
        cot_relay[c].start()
        cot_near[c].wait_recv()
        advance(c)
        cot_relay[c].wait_recv()
        whole = cotg[c]
        grad = mm(ot[...], whole).astype(bf16)
        for i in range(per):
            wb[c * per + i] = grad[:, i * uw : (i + 1) * uw]
        for i in range(per):
            progress[c * per + i] = 0
            reduce_step(c * per + i, 0)
        part = mm(w_ref[:, c * cw : (c + 1) * cw], whole, NT)
        if c == 0:
            dt32[...] = part
        else:
            dt32[...] += part
    for tile in range(4):
        with jax.named_scope(f'adv{tile}'):
            advance(units + tile)
        with jax.named_scope(f'bwd{tile}'):
            backward(tile)
    zero_pre = jnp.zeros((most - prefix, kvc), f32)
    pre = dkv[key_total : key_total + prefix, :]
    pre_full = jnp.concatenate([pre, zero_pre], axis=0)
    back_out[0] = jnp.where(b == 0, dkv[most + block : key_total, :], pre_full)
    back_out[1] = dkv[:most, :]
    backs = [
        remote(back_out.at[i], back_in.at[i], back_send.at[i], back_recv.at[i], (z, 1 - b, h))
        for i in range(2)
    ]
    for c in backs:
        c.start()
    turn = units + 4
    while min(progress) < 6:
        advance(turn)
        turn += 1
    for c in backs:
        c.wait_recv()
    head_part = dkv[most : 2 * most, :] + back_in[0] + jnp.where(b == 0, pre_full, 0.0)
    gkv_ref[:most, :] = head_part.astype(bf16)
    gkv_ref[most : block - most, :] = dkv[2 * most : block, :].astype(bf16)
    gkv_ref[block - most :, :] = (dkv[block : block + most, :] + back_in[1]).astype(bf16)
    for c in kv_copies + q_copies + cot_far + cot_near + cot_relay + backs:
        c.wait_send()
    for side, owner in ((0, 0), (1, 3)):
        @pl.when(h == owner)
        def _():
            for c in edge_copies(side):
                c.wait_send()
    for u in range(units):
        for k in range(6):
            reduce_copy(u, k).wait_send()


def publish_kernel(*refs):
    sems = refs[-1]
    count = (len(refs) - 1) // 2
    copies = [
        pltpu.make_async_copy(refs[i], refs[count + i], sems.at[i]) for i in range(count)
    ]
    for c in copies:
        c.start()
    for c in copies:
        c.wait()


def publish(arrays):
    done = pl.pallas_call(
        publish_kernel,
        out_shape=tuple(jax.ShapeDtypeStruct(a.shape, a.dtype) for a in arrays),
        in_specs=[pl.BlockSpec(memory_space=pltpu.VMEM)] * len(arrays),
        out_specs=(pl.BlockSpec(memory_space=pltpu.HBM),) * len(arrays),
        scratch_shapes=[pltpu.SemaphoreType.DMA((len(arrays),))],
        compiler_params=pltpu.CompilerParams(vmem_limit_bytes=8 * 1024 * 1024),
    )(*arrays)
    return tuple(a[None] for a in done[:-1]) + (done[-1],)


def on_device_fused(queries, keys_values, out_weight, cotangent, passage_lengths, causal_flags):
    chunks, units = 8, 8
    rows = queries.shape[1]
    block = 4 * rows
    seq = 2 * block
    most, prefix = seq // 16, seq // 32
    kvc = keys_values.shape[2] // 4
    hc = queries.shape[2] // 4
    hd = kvc // 2
    heads = hc // hd
    width = cotangent.shape[2]
    key_total = block + 2 * most
    window = rows + 2 * most + prefix
    vmem = pl.BlockSpec(memory_space=pltpu.VMEM)
    uw = width // units
    sem = pltpu.SemaphoreType.DMA
    attn, gq, gkv, gw = pl.pallas_call(
        functools.partial(fused_kernel, (rows, most, prefix, hd, heads, chunks, units)),
        out_shape=(
            jax.ShapeDtypeStruct((block, hc), bf16),
            jax.ShapeDtypeStruct((block, hc), bf16),
            jax.ShapeDtypeStruct((block, kvc), bf16),
            jax.ShapeDtypeStruct((hc, width), bf16),
        ),
        in_specs=[pl.BlockSpec(memory_space=pltpu.HBM)] * 4 + [vmem] * 2,
        out_specs=(vmem,) * 4,
        scratch_shapes=[
            pltpu.VMEM(queries.shape[1:], bf16),
            pltpu.VMEM(keys_values.shape[1:], bf16),
            pltpu.VMEM(out_weight.shape, bf16),
            sem((3 + chunks,)),
            pltpu.VMEM((block, hc), bf16),
            pltpu.VMEM((key_total, kvc), bf16),
            pltpu.VMEM((2, most, kvc), bf16),
            pltpu.VMEM((chunks, block, width // chunks), bf16),
            pltpu.VMEM((hc, block), bf16),
            pltpu.VMEM((hc, block), bf16),
            pltpu.VMEM((hc, block), f32),
            pltpu.VMEM((4, window, heads * rows), f32),
            pltpu.VMEM((key_total + prefix, kvc), f32),
            pltpu.VMEM((2, most, kvc), f32),
            pltpu.VMEM((2, most, kvc), f32),
            pltpu.VMEM((units, hc, uw), bf16),
            pltpu.VMEM((units, hc // 2, uw), bf16),
            pltpu.VMEM((units, hc // 4, uw), bf16),
            pltpu.VMEM((units, hc // 8, uw), bf16),
            sem((6,)),
            sem((6,)),
            sem((4,)),
            sem((2,)),
            sem((3 * chunks,)),
            sem((3 * chunks,)),
            sem((2,)),
            sem((2,)),
            sem((units * 6,)),
            sem((units * 6,)),
        ],
        compiler_params=pltpu.CompilerParams(
            collective_id=0, has_side_effects=True, vmem_limit_bytes=51 * 1024 * 1024
        ),
    )(
        queries[0], keys_values[0], out_weight, cotangent[0], passage_lengths, causal_flags
    )
    return publish((attn, gq, gkv, gw))


def fits(mesh):
    sizes = (mesh.shape["dp"], mesh.shape["blk"], mesh.shape["head"])
    return sizes == (4, 2, 4)


def solution(mesh):
    return jax.shard_map(
        on_device_fused if fits(mesh) else on_device,
        mesh=mesh,
        in_specs=(
            P("dp", ("blk", "head"), None),
            P("dp", ("blk", "head"), None),
            P("head", None),
            P("dp", ("blk", "head"), None),
            P("dp", None),
            P("dp", None),
        ),
        out_specs=(
            P("dp", "blk", "head"),
            P("dp", "blk", "head"),
            P("dp", "blk", "head"),
            P("head", None),
        ),
        check_vma=False,
    )
```

```python
import functools

import jax
import jax.numpy as jnp
from jax import lax
from jax.experimental import pallas as pl
from jax.experimental.pallas import tpu as pltpu
from jax.sharding import PartitionSpec as P

neg_fill = -1e30


def passed_along(value, axis, steps):
    count = lax.axis_size(axis)
    pairs = [(source, (source + steps) % count) for source in range(count)]
    return lax.ppermute(value, axis, pairs)


def describe(lengths, causal, positions, prefix):
    starts = prefix + jnp.cumsum(lengths) - lengths
    segment_id = jnp.sum((starts[None, :] <= positions[:, None]).astype(jnp.int32), axis=1)
    labels = jnp.arange(1, lengths.shape[0] + 1, dtype=jnp.int32)
    flag_of = jnp.sum(jnp.where(segment_id[:, None] == labels[None, :], causal[None, :], 0), axis=1)
    flag_of = flag_of + (segment_id == 0).astype(jnp.int32)
    return (segment_id, flag_of)


def permitted(query_info, key_info, query_pos, key_pos):
    query_seg, query_flag = query_info
    key_seg, key_flag = key_info
    same_list = query_seg[:, None] == key_seg[None, :]
    visible = same_list | (key_seg[None, :] == 0)
    ordered = (key_pos[None, :] <= query_pos[:, None]) | (query_flag[:, None] == 0) & same_list
    return visible & ordered


def on_device(queries, keys_values, out_weight, cotangent, passage_lengths, causal_flags):
    q_rows, kv_rows = (
        lax.all_to_all(queries[0], "head", split_axis=1, concat_axis=0, tiled=True),
        lax.all_to_all(keys_values[0], "head", split_axis=1, concat_axis=0, tiled=True),
    )
    local_rows = q_rows.shape[0]
    cycle_size = lax.axis_size("blk")
    own_index = lax.axis_index("blk")
    seq_total = local_rows * cycle_size
    prefix = seq_total // 32
    head_dim = kv_rows.shape[1] // 2
    head_count = q_rows.shape[1] // head_dim
    flat_rows = local_rows * head_count
    scale = head_dim ** (-0.5)
    lengths = passage_lengths[0]
    causal = causal_flags[0]
    query_pos = own_index * local_rows + jnp.arange(local_rows, dtype=jnp.int32)
    query_info = describe(lengths, causal, query_pos, prefix)
    q_flat = q_rows.reshape(flat_rows, head_dim)

    def allowed_for(key_start, span_rows, floor_pos, live):
        key_pos = key_start + jnp.arange(span_rows, dtype=jnp.int32)
        allowed = permitted(
            query_info, describe(lengths, causal, key_pos, prefix), query_pos, key_pos
        )
        allowed = allowed & (key_pos >= floor_pos)[None, :] & live
        expanded = jnp.broadcast_to(
            allowed[:, None, :], (local_rows, head_count, span_rows)
        ).reshape(flat_rows, span_rows)
        return (allowed, expanded)

    def score_block(key_block):
        return (
            lax.dot_general(
                q_flat,
                key_block[:, :head_dim],
                (((1,), (1,)), ((), ())),
                preferred_element_type=jnp.float32,
            )
            * scale
        )

    def visit(state, key_block, key_start, floor_pos, live):
        allowed, expanded = allowed_for(key_start, key_block.shape[0], floor_pos, live)

        def visit_compute(inner):
            running_max, totals = inner
            scores = score_block(key_block)
            block_max = jnp.max(jnp.where(expanded, scores, neg_fill), axis=1)
            new_best = jnp.maximum(running_max, block_max)
            factor = jnp.exp(running_max - new_best)
            weights = jnp.where(expanded, jnp.exp(scores - new_best[:, None]), 0.0)
            totals = totals * factor + jnp.sum(weights, axis=1)
            return (new_best, totals)

        def visit_keep(inner):
            return inner

        return lax.cond(jnp.any(allowed), visit_compute, visit_keep, state)

    state_start = (
        jnp.full((flat_rows,), neg_fill, jnp.float32),
        jnp.zeros((flat_rows,), jnp.float32),
    )
    always = jnp.array(True)
    initial = (jnp.zeros((seq_total, 2 * head_dim), jnp.bfloat16),) + state_start
    shard_rows = lax.all_gather(kv_rows, "blk", axis=0, tiled=True)

    def one_block(index, inner):
        key_block = lax.dynamic_slice_in_dim(shard_rows, index * local_rows, local_rows, 0)
        return visit(inner, key_block, index * local_rows, 0, always)

    inner = lax.fori_loop(0, shard_rows.shape[0] // local_rows, one_block, tuple(initial[1:]))
    stored, running_max, totals = (shard_rows,) + tuple(inner)
    log_norm = running_max + jnp.log(totals)

    def stored_rows(key_start, span_rows):
        return lax.dynamic_slice_in_dim(stored, key_start, span_rows, 0)

    def add_values(accum, key_block, key_start, floor_pos, live):
        allowed, expanded = allowed_for(key_start, key_block.shape[0], floor_pos, live)

        def add_compute(acc_in):
            scores = score_block(key_block)
            probs = jnp.where(expanded, jnp.exp(scores - log_norm[:, None]), 0.0)
            return acc_in + jnp.dot(
                probs.astype(jnp.bfloat16),
                key_block[:, head_dim:],
                preferred_element_type=jnp.float32,
            )

        def add_keep(acc_in):
            return acc_in

        return lax.cond(jnp.any(allowed), add_compute, add_keep, accum)

    accum = jnp.zeros((flat_rows, head_dim), jnp.float32)

    def value_turn(index, acc_in):
        return add_values(
            acc_in, stored_rows(index * local_rows, local_rows), index * local_rows, 0, always
        )

    accum = lax.fori_loop(0, cycle_size, value_turn, accum)
    attn = accum.reshape(local_rows, head_count * head_dim).astype(jnp.bfloat16)
    project_shard_rows = lax.all_gather(cotangent[0], "head", axis=0, tiled=True)
    product = lax.dot_general(
        project_shard_rows, out_weight, (((1,), (1,)), ((), ())), preferred_element_type=jnp.float32
    )
    grads = product
    weight_acc = lax.dot_general(
        attn, project_shard_rows, (((0,), (0,)), ((), ())), preferred_element_type=jnp.float32
    )
    grads, weight_acc = (grads, weight_acc)
    attention_gradient = grads.astype(jnp.bfloat16)
    d_flat = attention_gradient.reshape(flat_rows, head_dim)
    row_dot = jnp.sum(
        (attention_gradient.astype(jnp.float32) * attn.astype(jnp.float32)).reshape(
            flat_rows, head_dim
        ),
        axis=1,
    )
    shares = lax.psum_scatter(
        weight_acc.astype(jnp.bfloat16), "blk", scatter_dimension=1, tiled=True
    ).astype(jnp.float32)
    shares = lax.psum(shares.astype(jnp.bfloat16), "dp")
    grad_weight = lax.all_gather(shares, "blk", axis=1, tiled=True)

    def contribute(grad_q, key_block, key_start, floor_pos, live):
        span_rows = key_block.shape[0]
        allowed, expanded = allowed_for(key_start, span_rows, floor_pos, live)

        def contribute_compute(grad_in):
            scores = score_block(key_block)
            probs = jnp.where(expanded, jnp.exp(scores - log_norm[:, None]), 0.0)
            dprob = lax.dot_general(
                d_flat,
                key_block[:, head_dim:],
                (((1,), (1,)), ((), ())),
                preferred_element_type=jnp.float32,
            )
            dscore = (probs * (dprob - row_dot[:, None])).astype(jnp.bfloat16)
            grad_out = grad_in + scale * jnp.dot(
                dscore, key_block[:, :head_dim], preferred_element_type=jnp.float32
            )
            grad_key = scale * lax.dot_general(
                dscore, q_flat, (((0,), (0,)), ((), ())), preferred_element_type=jnp.float32
            )
            grad_value = lax.dot_general(
                probs.astype(jnp.bfloat16),
                d_flat,
                (((0,), (0,)), ((), ())),
                preferred_element_type=jnp.float32,
            )
            return (grad_out, jnp.concatenate([grad_key, grad_value], axis=1))

        def skip(grad_in):
            return (grad_in, jnp.zeros((span_rows, 2 * head_dim), jnp.float32))

        return lax.cond(jnp.any(allowed), contribute_compute, skip, grad_q)

    grad_start = jnp.zeros((flat_rows, head_dim), jnp.float32)

    def turn_single(turn_index, state):
        grad_q, passing = state
        target = (own_index - 1 - turn_index) % cycle_size
        grad_q, piece_grad = contribute(
            grad_q, stored_rows(target * local_rows, local_rows), target * local_rows, 0, always
        )
        passing = passed_along((passing + piece_grad).astype(jnp.bfloat16), "blk", 1).astype(
            jnp.float32
        )
        return (grad_q, passing)

    zero_full = jnp.zeros((local_rows, 2 * head_dim), jnp.float32)
    grad_q, passing = lax.fori_loop(0, cycle_size - 1, turn_single, (grad_start, zero_full))
    grad_q, piece_grad = contribute(
        grad_q, stored_rows(own_index * local_rows, local_rows), own_index * local_rows, 0, always
    )
    key_value_gradient = passing + piece_grad
    grad_queries = grad_q.reshape(local_rows, head_count * head_dim).astype(jnp.bfloat16)
    return (
        attn[None],
        grad_queries[None],
        key_value_gradient.astype(jnp.bfloat16)[None],
        grad_weight,
    )


MESH = pl.DeviceIdType.MESH
f32, bf16 = jnp.float32, jnp.bfloat16
NN = (((1,), (0,)), ((), ()))
NT = (((1,), (1,)), ((), ()))


def mm(a, b, dims=NN):
    return lax.dot_general(a, b, dims, preferred_element_type=f32)


def fused_kernel(
    sizes,
    q_hbm,
    kv_hbm,
    w_hbm,
    cot_hbm,
    len_ref,
    flag_ref,
    attn_ref,
    gq_ref,
    gkv_ref,
    gw_ref,
    q_ref,
    kv_ref,
    w_ref,
    local_sem,
    qg,
    kvl,
    edge,
    cotg,
    qt,
    ot,
    dt32,
    probs,
    dkv,
    back_out,
    back_in,
    wb,
    r0,
    r1,
    r2,
    qkv_send,
    qkv_recv,
    edge_send,
    edge_recv,
    cot_send,
    cot_recv,
    back_send,
    back_recv,
    red_send,
    red_recv,
):
    rows, most, prefix, hd, heads, chunks, units = sizes
    z, b, h = lax.axis_index("dp"), lax.axis_index("blk"), lax.axis_index("head")
    block = 4 * rows
    seq = 2 * block
    hc = heads * hd
    kvc = 2 * hd
    span = rows + 2 * most
    width = cot_hbm.shape[1]
    cw = width // chunks
    uw = width // units
    h1 = h + 1 - 2 * lax.rem(h, 2)
    h2 = lax.rem(h + 2, 4)
    h3 = 3 - h
    peers = (h1, h2, h3)
    za = z + 1 - 2 * lax.rem(z, 2)
    zb = lax.rem(z + 2, 4)
    bit_a = lax.rem(z, 2)
    bit_b = z // 2
    partners = (((za, b, h), bit_a), ((zb, b, h), bit_b), ((z, 1 - b, h), b))

    barrier = pltpu.get_barrier_semaphore()
    others = [(z, b, p) for p in peers] + [(z, 1 - b, p) for p in (h, h1, h2, h3)]
    others += [(za, b, h), (zb, b, h)]
    for who in others:
        pl.semaphore_signal(barrier, inc=1, device_id=who, device_id_type=MESH)

    def at(index, size):
        return pl.ds(pl.multiple_of(index * size, size), size)

    def remote(src, dst, send, recv, who):
        return pltpu.make_async_remote_copy(
            src_ref=src, dst_ref=dst, send_sem=send, recv_sem=recv,
            device_id=who, device_id_type=MESH,
        )

    loads = [
        pltpu.make_async_copy(kv_hbm, kv_ref, local_sem.at[0]),
        pltpu.make_async_copy(q_hbm, q_ref, local_sem.at[1]),
    ]
    for c in range(chunks):
        loads.append(pltpu.make_async_copy(
            cot_hbm.at[:, pl.ds(c * cw, cw)], cotg.at[c, at(h, rows)], local_sem.at[3 + c]))
    loads.append(pltpu.make_async_copy(w_hbm, w_ref, local_sem.at[2]))
    for c in loads:
        c.start()
    pl.semaphore_wait(barrier, len(others))

    kv_rows = pl.ds(pl.multiple_of(most + h * rows, most), rows)
    kv_copies, q_copies = [], []
    for i, p in ((1, h2), (2, h3), (0, h1)):
        kv_copies.append(remote(
            kv_ref.at[:, at(p, kvc)], kvl.at[kv_rows],
            qkv_send.at[i], qkv_recv.at[i], (z, b, p)))
        q_copies.append(remote(
            q_ref.at[:, at(p, hc)], qg.at[at(h, rows)],
            qkv_send.at[3 + i], qkv_recv.at[3 + i], (z, b, p)))

    def edge_copies(side):
        first = 0 if side == 0 else rows - most
        return [
            remote(
                kv_ref.at[pl.ds(first, most), at(p, kvc)], edge.at[side],
                edge_send.at[j], edge_recv.at[side], (z, 1 - b, p))
            for j, p in enumerate((h2, h3, h, h1))
        ]

    loads[0].wait()
    for c in kv_copies:
        c.start()
    for side, owner in ((0, 0), (1, 3)):
        @pl.when(h == owner)
        def _():
            for c in edge_copies(side):
                c.start()
    loads[1].wait()
    for c in q_copies:
        c.start()
    cot_far, cot_near, cot_relay = [], [], []
    for c in range(chunks):
        piece = cotg.at[c, at(h, rows)]
        cot_far.append(remote(
            piece, cotg.at[c, at(h, rows)], cot_send.at[c], cot_recv.at[c], (z, b, h2)))
        cot_near.append(remote(
            piece, cotg.at[c, at(h, rows)], cot_send.at[chunks + c],
            cot_recv.at[chunks + c], (z, b, h1)))
        cot_relay.append(remote(
            cotg.at[c, at(h2, rows)], cotg.at[c, at(h2, rows)],
            cot_send.at[2 * chunks + c], cot_recv.at[2 * chunks + c], (z, b, h1)))
    for c in range(chunks):
        loads[2 + c].wait()
        cot_far[c].start()
        cot_near[c].start()

    qg[at(h, rows), :] = q_ref[:, at(h, hc)]
    kvl[kv_rows, :] = kv_ref[:, at(h, kvc)]
    dkv[...] = jnp.zeros_like(dkv)

    lists = len_ref.shape[1]
    len_row = len_ref[...].astype(f32)
    flag_row = flag_ref[...].astype(f32)
    ii = lax.broadcasted_iota(jnp.int32, (lists, lists), 0)
    jj = lax.broadcasted_iota(jnp.int32, (lists, lists), 1)
    len_col = jnp.sum(jnp.where(ii == jj, len_row, 0.0), axis=1, keepdims=True)
    flag_col = jnp.sum(jnp.where(ii == jj, flag_row, 0.0), axis=1, keepdims=True)
    start_col = prefix + jnp.sum(jnp.where(jj < ii, len_row, 0.0), axis=1, keepdims=True)
    start_row = prefix + jnp.sum(jnp.where(ii < jj, len_col, 0.0), axis=0, keepdims=True)
    base = (b * block).astype(f32)
    key_total = block + 2 * most
    kpos = lax.broadcasted_iota(jnp.int32, (key_total, 1), 0).astype(f32) + (base - most)
    kseg = jnp.sum(jnp.where(start_row <= kpos, 1.0, 0.0), axis=1, keepdims=True)
    kseg = jnp.where((kpos < prefix) | (kpos >= seq), -1.0, kseg)
    ppos = lax.broadcasted_iota(jnp.int32, (prefix, 1), 0).astype(f32)
    pseg = jnp.zeros((prefix, 1), f32)
    qpos = lax.broadcasted_iota(jnp.int32, (1, block), 1).astype(f32) + base
    qseg = jnp.sum(jnp.where(start_col <= qpos, 1.0, 0.0), axis=0, keepdims=True)
    label = lax.broadcasted_iota(jnp.int32, (lists, 1), 0).astype(f32) + 1.0
    qflag = jnp.sum(jnp.where(label == qseg, flag_col, 0.0), axis=0, keepdims=True)
    qflag = qflag + jnp.where(qseg == 0.0, 1.0, 0.0)

    for c in kv_copies:
        c.wait_recv()
    for side in range(2):
        edge_copies(side)[0].wait_recv()
    first = jnp.where(b == 0, kvl[most : most + prefix, :], edge[0, :prefix, :])
    kvl[:most, :] = jnp.where(b == 0, jnp.zeros_like(edge[1]), edge[1])
    kvl[most + block :, :] = jnp.where(b == 0, edge[0], jnp.zeros_like(edge[0]))
    for c in q_copies:
        c.wait_recv()
    qt[...] = (qg[...].astype(f32) * (hd ** -0.5)).T.astype(bf16)
    blank = jnp.zeros((hd, heads * rows), bf16)

    def lanes(ref, tile):
        return jnp.concatenate(
            [ref[i * hd : (i + 1) * hd, tile * rows : (tile + 1) * rows] for i in range(heads)],
            axis=1,
        )

    def stacked(value):
        return jnp.concatenate(
            [value[:, i * rows : (i + 1) * rows] for i in range(heads)], axis=0
        )

    def window(tile):
        return jnp.concatenate([kvl[tile * rows : tile * rows + span, :], first], axis=0)

    def forward(tile):
        kw = window(tile)
        scores = mm(kw, jnp.concatenate([lanes(qt, tile), blank], axis=0))
        cut = slice(tile * rows, tile * rows + span)
        kp = jnp.concatenate([kpos[cut], ppos], axis=0)
        ks = jnp.concatenate([kseg[cut], pseg], axis=0)
        sl = slice(tile * rows, (tile + 1) * rows)
        qp, qs, qf = qpos[:, sl], qseg[:, sl], qflag[:, sl]
        same = ks == qs
        allowed = (same | (ks == 0.0)) & ((kp <= qp) | ((qf == 0.0) & same))
        fill = jnp.where(allowed, 0.0, neg_fill)
        scores = scores + jnp.concatenate([fill] * heads, axis=1)
        best = jnp.max(scores, axis=0, keepdims=True)
        e = jnp.exp(scores - best)
        p = e * (1.0 / jnp.sum(e, axis=0, keepdims=True))
        probs[tile] = p
        out = stacked(mm(kw.T[hd:], p.astype(bf16)))
        ot[:, sl] = out.astype(bf16)
        attn_ref[sl, :] = out.T.astype(bf16)

    def backward(tile):
        kw = window(tile)
        sl = slice(tile * rows, (tile + 1) * rows)
        p = probs[tile]
        d = lanes(dt32, tile).astype(bf16)
        o = lanes(ot, tile)
        row_dot = jnp.sum(d.astype(f32) * o.astype(f32), axis=0, keepdims=True)
        d_pad = jnp.concatenate([blank, d], axis=0)
        q_pad = jnp.concatenate([lanes(qt, tile), blank], axis=0)
        ds = (p * (mm(kw, d_pad) - row_dot)).astype(bf16)
        gq = stacked(mm(kw.T[:hd], ds)) * (hd ** -0.5)
        gq_ref[sl, :] = gq.T.astype(bf16)
        both = mm(ds, q_pad, NT) + mm(p.astype(bf16), d_pad, NT)
        cut = slice(tile * rows, tile * rows + span)
        dkv[cut, :] += both[:span]
        tail = slice(key_total, key_total + prefix)
        dkv[tail, :] += both[span:]

    def order(u):
        near, far, side = partners
        return (near, side, far) if u % 3 == 1 else (side, near, far)

    def reduce_copy(u, k):
        dims = order(u)
        size = hc
        keep = []
        low = 0
        for _, bit in dims:
            size = size // 2
            low = low + bit * size
            keep.append((low, size))
        sems = (red_send.at[u * 6 + k], red_recv.at[u * 6 + k])
        if k < 3:
            who, bit = dims[k]
            low, size = keep[k]
            away = low + (1 - 2 * bit) * size
            src = wb.at[u, pl.ds(pl.multiple_of(away, size), size)]
            return remote(src, (r0, r1, r2)[k].at[u], *sems, who)
        low, size = keep[5 - k]
        part = gw_ref.at[pl.ds(pl.multiple_of(low, size), size), pl.ds(u * uw, uw)]
        return remote(part, part, *sems, dims[5 - k][0])

    def reduce_step(u, k):
        if k > 0:
            reduce_copy(u, k - 1).wait_recv()
        if 0 < k < 4:
            dims = order(u)
            low, size = 0, hc
            for _, bit in dims[:k]:
                size = size // 2
                low = low + bit * size
            at_rows = pl.ds(pl.multiple_of(low, size), size)
            total = wb[u, at_rows, :].astype(f32) + (r0, r1, r2)[k - 1][u].astype(f32)
            if k < 3:
                wb[u, at_rows, :] = total.astype(bf16)
            else:
                gw_ref[at_rows, u * uw : (u + 1) * uw] = total.astype(bf16)
        if k < 6:
            reduce_copy(u, k).start()

    progress = [-1] * units

    def advance(turn):
        ranked = range(units) if turn < units else reversed(range(units))
        for u in ranked:
            if 0 <= progress[u] < 5 and turn - u >= 3 and (turn - u) % 2 == 1:
                progress[u] += 1
                reduce_step(u, progress[u])

    loads[2 + chunks].wait()
    per = units // chunks
    for tile in range(4):
        with jax.named_scope(f'fwd{tile}'):
            forward(tile)
    for c in range(chunks):
        cot_far[c].wait_recv()
        cot_relay[c].start()
        cot_near[c].wait_recv()
        advance(c)
        cot_relay[c].wait_recv()
        whole = cotg[c]
        grad = mm(ot[...], whole).astype(bf16)
        for i in range(per):
            wb[c * per + i] = grad[:, i * uw : (i + 1) * uw]
        for i in range(per):
            progress[c * per + i] = 0
            reduce_step(c * per + i, 0)
        part = mm(w_ref[:, c * cw : (c + 1) * cw], whole, NT)
        if c == 0:
            dt32[...] = part
        else:
            dt32[...] += part
    for tile in range(4):
        with jax.named_scope(f'adv{tile}'):
            advance(units + tile)
        with jax.named_scope(f'bwd{tile}'):
            backward(tile)
    zero_pre = jnp.zeros((most - prefix, kvc), f32)
    pre = dkv[key_total : key_total + prefix, :]
    pre_full = jnp.concatenate([pre, zero_pre], axis=0)
    back_out[0] = jnp.where(b == 0, dkv[most + block : key_total, :], pre_full)
    back_out[1] = dkv[:most, :]
    backs = [
        remote(back_out.at[i], back_in.at[i], back_send.at[i], back_recv.at[i], (z, 1 - b, h))
        for i in range(2)
    ]
    for c in backs:
        c.start()
    turn = units + 4
    while min(progress) < 5:
        advance(turn)
        turn += 1
    for u in range(units):
        reduce_step(u, 6)
    for c in backs:
        c.wait_recv()
    head_part = dkv[most : 2 * most, :] + back_in[0] + jnp.where(b == 0, pre_full, 0.0)
    gkv_ref[:most, :] = head_part.astype(bf16)
    gkv_ref[most : block - most, :] = dkv[2 * most : block, :].astype(bf16)
    gkv_ref[block - most :, :] = (dkv[block : block + most, :] + back_in[1]).astype(bf16)
    for c in kv_copies + q_copies + cot_far + cot_near + cot_relay + backs:
        c.wait_send()
    for side, owner in ((0, 0), (1, 3)):
        @pl.when(h == owner)
        def _():
            for c in edge_copies(side):
                c.wait_send()
    for u in range(units):
        for k in range(6):
            reduce_copy(u, k).wait_send()


def publish_kernel(*refs):
    sems = refs[-1]
    count = (len(refs) - 1) // 2
    copies = [
        pltpu.make_async_copy(refs[i], refs[count + i], sems.at[i]) for i in range(count)
    ]
    for c in copies:
        c.start()
    for c in copies:
        c.wait()


def publish(arrays):
    done = pl.pallas_call(
        publish_kernel,
        out_shape=tuple(jax.ShapeDtypeStruct(a.shape, a.dtype) for a in arrays),
        in_specs=[pl.BlockSpec(memory_space=pltpu.VMEM)] * len(arrays),
        out_specs=(pl.BlockSpec(memory_space=pltpu.HBM),) * len(arrays),
        scratch_shapes=[pltpu.SemaphoreType.DMA((len(arrays),))],
        compiler_params=pltpu.CompilerParams(vmem_limit_bytes=8 * 1024 * 1024),
    )(*arrays)
    return tuple(a[None] for a in done[:-1]) + (done[-1],)


def on_device_fused(queries, keys_values, out_weight, cotangent, passage_lengths, causal_flags):
    chunks, units = 8, 8
    rows = queries.shape[1]
    block = 4 * rows
    seq = 2 * block
    most, prefix = seq // 16, seq // 32
    kvc = keys_values.shape[2] // 4
    hc = queries.shape[2] // 4
    hd = kvc // 2
    heads = hc // hd
    width = cotangent.shape[2]
    key_total = block + 2 * most
    window = rows + 2 * most + prefix
    vmem = pl.BlockSpec(memory_space=pltpu.VMEM)
    uw = width // units
    sem = pltpu.SemaphoreType.DMA
    attn, gq, gkv, gw = pl.pallas_call(
        functools.partial(fused_kernel, (rows, most, prefix, hd, heads, chunks, units)),
        out_shape=(
            jax.ShapeDtypeStruct((block, hc), bf16),
            jax.ShapeDtypeStruct((block, hc), bf16),
            jax.ShapeDtypeStruct((block, kvc), bf16),
            jax.ShapeDtypeStruct((hc, width), bf16),
        ),
        in_specs=[pl.BlockSpec(memory_space=pltpu.HBM)] * 4 + [vmem] * 2,
        out_specs=(vmem,) * 4,
        scratch_shapes=[
            pltpu.VMEM(queries.shape[1:], bf16),
            pltpu.VMEM(keys_values.shape[1:], bf16),
            pltpu.VMEM(out_weight.shape, bf16),
            sem((3 + chunks,)),
            pltpu.VMEM((block, hc), bf16),
            pltpu.VMEM((key_total, kvc), bf16),
            pltpu.VMEM((2, most, kvc), bf16),
            pltpu.VMEM((chunks, block, width // chunks), bf16),
            pltpu.VMEM((hc, block), bf16),
            pltpu.VMEM((hc, block), bf16),
            pltpu.VMEM((hc, block), f32),
            pltpu.VMEM((4, window, heads * rows), f32),
            pltpu.VMEM((key_total + prefix, kvc), f32),
            pltpu.VMEM((2, most, kvc), f32),
            pltpu.VMEM((2, most, kvc), f32),
            pltpu.VMEM((units, hc, uw), bf16),
            pltpu.VMEM((units, hc // 2, uw), bf16),
            pltpu.VMEM((units, hc // 4, uw), bf16),
            pltpu.VMEM((units, hc // 8, uw), bf16),
            sem((6,)),
            sem((6,)),
            sem((4,)),
            sem((2,)),
            sem((3 * chunks,)),
            sem((3 * chunks,)),
            sem((2,)),
            sem((2,)),
            sem((units * 6,)),
            sem((units * 6,)),
        ],
        compiler_params=pltpu.CompilerParams(
            collective_id=0, has_side_effects=True, vmem_limit_bytes=51 * 1024 * 1024
        ),
    )(
        queries[0], keys_values[0], out_weight, cotangent[0], passage_lengths, causal_flags
    )
    return publish((attn, gq, gkv, gw))


def fits(mesh):
    sizes = (mesh.shape["dp"], mesh.shape["blk"], mesh.shape["head"])
    return sizes == (4, 2, 4)


def solution(mesh):
    return jax.shard_map(
        on_device_fused if fits(mesh) else on_device,
        mesh=mesh,
        in_specs=(
            P("dp", ("blk", "head"), None),
            P("dp", ("blk", "head"), None),
            P("head", None),
            P("dp", ("blk", "head"), None),
            P("dp", None),
            P("dp", None),
        ),
        out_specs=(
            P("dp", "blk", "head"),
            P("dp", "blk", "head"),
            P("dp", "blk", "head"),
            P("head", None),
        ),
        check_vma=False,
    )
```
